128 devices in a mesh: gx: 4 (over y), gy: 32 (over x, z, core).
Axes of the slice: x: 4, y: 4, z: 4, core: 2. Of those that a mesh axis runs over, the one named last changes fastest.
Arguments:
- vertex_state: bfloat16 [1024, 256, 128], P(('gx', 'gy')), may hold values from -6 to 6
- edge_state: bfloat16 [1024, 1536, 128], P(('gx', 'gy')), may hold values from -6 to 6
- senders: int32 [1024, 1536], P(('gx', 'gy')), may hold values from 0 to 511
- receivers: int32 [1024, 1536], P(('gx', 'gy')), may hold values from 0 to 255
- counts: int32 [1024], P(('gx', 'gy')), may hold values from 768 to 1536
- border_rows: int32 [1024, 2, 128], P(('gx', 'gy')), may hold values from 0 to 255
- old_neighbours: int32 [1024, 2], P(('gx', 'gy')), may hold values from 0 to 1023, as said below
- new_neighbours: int32 [1024, 2], P(('gx', 'gy')), may hold values from 0 to 1023, as said below
- new_place: int32 [1024], P(('gx', 'gy')), may hold values from 0 to 1023, as said below
- weights_in: bfloat16 [3, 5, 128, 128], replicated, may hold values from -0.5 to 0.5
- weights_out: bfloat16 [3, 2, 128, 128], replicated, may hold values from -0.5 to 0.5
- biases: float32 [3, 6, 128], replicated, may hold values from -3 to 3
- norm_gains: float32 [3, 2, 128], replicated, may hold values from 0.25 to 1.75
Outputs:
- vertex_out: bfloat16 [1024, 256, 128], P(('gx', 'gy'))
- edge_out: bfloat16 [1024, 1536, 128], P(('gx', 'gy'))
The draws below stay inside these ranges and needn't reach their ends.
Inputs may be any that keep to these rules, and one draw needn't show every extreme that they name: A permutation of the patches. With devices numbered gx-index times the size of gy plus gy-index, patch p stands on device p // 8 and moves to device new_place[p] // 8, which has the same gx-index; one device sends at most 1 patch to any one device, and some pair of devices reaches 1. old_neighbours[p, 0] stands on the device whose gy-index is one less than that of p's device (cyclically) and whose gx-index is the same; old_neighbours[p, 1] on the device whose gx-index is one less (cyclically) and whose gy-index is the same. new_neighbours[new_place[p], k] = new_place[old_neighbours[p, k]]; in the new positions it follows the same rule as old_neighbours.
All inputs are finite; a program needn't handle non-finite values.
Results may differ from the reference program's by a relative error of at most 0.0066.
Values may be sent and summed in bfloat16 or wider, within the bound.
No kernel may reach another device: no remote copies, remote signals or barrier semaphores. Data moves between devices by JAX's collectives and lax.ppermute only.
A program may use at most 128 MiB of HBM per device.

```python
import jax
import jax.numpy as jnp
from jax import lax

WIDTH = 128
VERTS = 256
EDGES = 1536
BORDER = 128
PATCH_DEV = 8
STEPS_OLD = 2
STEPS_NEW = 1
STEPS = 3
PATCHES = 1024
N_GX = 4
N_GY = 32


def patch_layout(key):
    seed_base = jax.random.fold_in(key, 4242)
    shift_key, old_key, new_key = jax.random.split(seed_base, 3)
    capacity = (PATCH_DEV + N_GY - 1) // N_GY
    raw_offsets = (jax.random.permutation(shift_key, N_GY * capacity)[:PATCH_DEV] // capacity).astype(jnp.int32)
    offsets = ((raw_offsets - raw_offsets[0] + N_GY // 2) % N_GY).astype(jnp.int32)
    device_total = N_GX * N_GY
    old_slots = jax.vmap(lambda sub_key: jax.random.permutation(sub_key, PATCH_DEV))(jax.random.split(old_key, device_total)).reshape(N_GX, N_GY, PATCH_DEV).astype(jnp.int32)
    new_slots = jax.vmap(lambda sub_key: jax.random.permutation(sub_key, PATCH_DEV))(jax.random.split(new_key, device_total)).reshape(N_GX, N_GY, PATCH_DEV).astype(jnp.int32)
    along_x = jnp.arange(N_GX, dtype=jnp.int32)[:, None, None]
    along_y = jnp.arange(N_GY, dtype=jnp.int32)[None, :, None]
    tracks = jnp.arange(PATCH_DEV, dtype=jnp.int32)[None, None, :]

    def old_position(row_x, row_y):
        row_x = row_x % N_GX
        row_y = row_y % N_GY
        return (row_x * N_GY + row_y) * PATCH_DEV + old_slots[row_x, row_y, tracks]

    def new_position(row_x, row_y):
        row_x = row_x % N_GX
        landing = (row_y + offsets[tracks]) % N_GY
        return (row_x * N_GY + landing) * PATCH_DEV + new_slots[row_x, landing, tracks]
    old_spots = old_position(along_x, along_y).reshape(-1)
    new_spots = new_position(along_x, along_y).reshape(-1)
    patch_total = device_total * PATCH_DEV
    place_table = jnp.zeros((patch_total,), jnp.int32).at[old_spots].set(new_spots)
    old_links = jnp.stack([old_position(along_x, along_y - 1), old_position(along_x - 1, along_y)], axis=-1).reshape(-1, 2)
    new_links = jnp.stack([new_position(along_x, along_y - 1), new_position(along_x - 1, along_y)], axis=-1).reshape(-1, 2)
    old_table = jnp.zeros((patch_total, 2), jnp.int32).at[old_spots].set(old_links)
    new_table = jnp.zeros((patch_total, 2), jnp.int32).at[new_spots].set(new_links)
    return (place_table, old_table, new_table)


def draw_new_place(key, part):
    return patch_layout(key)[0]


def draw_old_neighbours(key, part):
    return patch_layout(key)[1]


def draw_new_neighbours(key, part):
    return patch_layout(key)[2]


def touch_ends(entries, key, least, largest):
    longest = entries.shape.index(max(entries.shape))
    spots = []
    for shift in (0, 1):
        where = [jax.random.randint(jax.random.fold_in(key, axis), (), 0, length) for axis, length in enumerate(entries.shape)]
        where[longest] = (where[longest] + shift) % entries.shape[longest]
        spots.append(tuple(where))
    return entries.at[spots[0]].set(least).at[spots[1]].set(largest)


def block_scale(stream_key, dims, cuts, least, top_value):
    def one(position, blocks):
        steps = jax.random.uniform(jax.random.fold_in(jax.random.fold_in(stream_key, 6), position), (blocks,), jnp.float32, least / len(cuts), top_value / len(cuts))
        return jnp.repeat(jnp.exp(steps), dims[position] // blocks).reshape((-1,) + (1,) * (len(dims) - position - 1))

    gain = one(*cuts[0])
    for cut in cuts[1:]:
        gain = gain * one(*cut)
    return gain


def noise(key, shape, scale, most, cuts=(), held_as=jnp.bfloat16):
    loudness = block_scale(key, shape, cuts, -0.22, 0.18) if cuts else 1.0
    values = jax.random.normal(key, shape, jnp.float32) * scale * loudness
    return jnp.minimum(jnp.maximum(values, -most), most).astype(held_as)


def setup_inputs(seed: int = 0) -> dict:
    key_of = jax.random.split(jax.random.key(seed), 14)
    return {
        "vertex_state": noise(key_of[0], (PATCHES, VERTS, WIDTH), 1.0, 6.0, ((0, 128),)),
        "edge_state": noise(key_of[1], (PATCHES, EDGES, WIDTH), 1.0, 6.0, ((0, 128),)),
        "senders": touch_ends(jax.random.randint(key_of[2], (PATCHES, EDGES), 0, VERTS + 2 * BORDER), jax.random.fold_in(key_of[2], 1), 0, (VERTS + 2 * BORDER) - 1).astype(jnp.int32),
        "receivers": touch_ends(jax.random.randint(key_of[3], (PATCHES, EDGES), 0, VERTS), jax.random.fold_in(key_of[3], 1), 0, VERTS - 1).astype(jnp.int32),
        "counts": touch_ends(jax.random.randint(key_of[4], (PATCHES,), EDGES // 2, EDGES + 1), jax.random.fold_in(key_of[4], 1), EDGES // 2, EDGES).astype(jnp.int32),
        "border_rows": touch_ends(jax.random.randint(key_of[5], (PATCHES, 2, BORDER), 0, VERTS), jax.random.fold_in(key_of[5], 1), 0, VERTS - 1).astype(jnp.int32),
        "old_neighbours": draw_old_neighbours(jax.random.fold_in(key_of[13], 71), 0),
        "new_neighbours": draw_new_neighbours(jax.random.fold_in(key_of[13], 71), 0),
        "new_place": draw_new_place(jax.random.fold_in(key_of[13], 71), 0),
        "weights_in": noise(key_of[9], (STEPS, 5, WIDTH, WIDTH), WIDTH ** -0.5, 0.5),
        "weights_out": noise(key_of[10], (STEPS, 2, WIDTH, WIDTH), WIDTH ** -0.5, 0.5),
        "biases": noise(key_of[11], (STEPS, 6, WIDTH), 0.5, 3.0, (), jnp.float32),
        "norm_gains": jnp.clip(1.0 + 0.15 * jax.random.normal(key_of[12], (STEPS, 2, WIDTH), jnp.float32), 0.25, 1.75),
    }


def product(left, right):
    return jnp.dot(left, right, preferred_element_type=jnp.float32)

def normalize(values, scale_row, shift_row):
    center = values - lax.optimization_barrier(jnp.mean(values, axis=-1, keepdims=True))
    spread = lax.optimization_barrier(jnp.mean(center * center, axis=-1, keepdims=True))
    return center * lax.rsqrt(spread + 1e-05) * scale_row + shift_row

def ghost_rows(vertex_state, border_rows, neighbours):
    patch_rows = jnp.arange(vertex_state.shape[0], dtype=jnp.int32)[:, None]
    along_gy = vertex_state[patch_rows, border_rows[:, 0]]
    along_gx = vertex_state[patch_rows, border_rows[:, 1]]
    return jnp.concatenate([along_gy[neighbours[:, 0]], along_gx[neighbours[:, 1]]], axis=1)

def patch_update(layer_weights, pieces):
    weights_in, weights_out, bias_rows, gain_rows = layer_weights
    vertex_block, ghost_block, edge_block, sender_ids, receiver_ids, edge_count = pieces
    vertex_count = vertex_block.shape[0]
    edge_total = edge_block.shape[0]
    joined = jnp.concatenate([vertex_block, ghost_block], axis=0)
    sender_terms = product(joined, weights_in[1]).astype(jnp.bfloat16)
    receiver_terms = product(vertex_block, weights_in[2]).astype(jnp.bfloat16)
    summed = product(edge_block, weights_in[0]) + sender_terms[sender_ids].astype(jnp.float32)
    summed = summed + receiver_terms[receiver_ids].astype(jnp.float32) + bias_rows[0]
    edge_hidden = jax.nn.relu(summed).astype(jnp.bfloat16)
    edge_update = normalize(product(edge_hidden, weights_out[0]) + bias_rows[1], gain_rows[0], bias_rows[2])
    live = jnp.arange(edge_total, dtype=jnp.int32) < edge_count
    widened = edge_block.astype(jnp.float32)
    fresh_edges = jnp.where(live[:, None], widened + edge_update, widened).astype(jnp.bfloat16)
    masked = jnp.where(live[:, None], fresh_edges.astype(jnp.float32), jnp.zeros_like(widened))
    aggregate = jax.ops.segment_sum(masked, receiver_ids, num_segments=vertex_count).astype(jnp.bfloat16)
    node_hidden = product(vertex_block, weights_in[3]) + product(aggregate, weights_in[4]) + bias_rows[3]
    node_hidden = jax.nn.relu(node_hidden).astype(jnp.bfloat16)
    vertex_update = normalize(product(node_hidden, weights_out[1]) + bias_rows[4], gain_rows[1], bias_rows[5])
    fresh_vertices = (vertex_block.astype(jnp.float32) + vertex_update).astype(jnp.bfloat16)
    return (fresh_vertices, fresh_edges)

def full_step(layer_weights, vertex_state, edge_state, senders, receivers, counts, border_rows, neighbours):
    ghosts = ghost_rows(vertex_state, border_rows, neighbours)
    return lax.map(lambda pieces: patch_update(layer_weights, pieces), (vertex_state, ghosts, edge_state, senders, receivers, counts))

def relocate(values, new_place):
    return jnp.zeros_like(values).at[new_place].set(values)

def reference(vertex_state, edge_state, senders, receivers, counts, border_rows, old_neighbours, new_neighbours, new_place, weights_in, weights_out, biases, norm_gains):
    for step_index in range(STEPS_OLD):
        layer_weights = (weights_in[step_index], weights_out[step_index], biases[step_index], norm_gains[step_index])
        vertex_state, edge_state = full_step(layer_weights, vertex_state, edge_state, senders, receivers, counts, border_rows, old_neighbours)
    vertex_state = relocate(vertex_state, new_place)
    edge_state = relocate(edge_state, new_place)
    senders = relocate(senders, new_place)
    receivers = relocate(receivers, new_place)
    counts = relocate(counts, new_place)
    border_rows = relocate(border_rows, new_place)
    for step_index in range(STEPS_NEW):
        which = STEPS_OLD + step_index
        layer_weights = (weights_in[which], weights_out[which], biases[which], norm_gains[which])
        vertex_state, edge_state = full_step(layer_weights, vertex_state, edge_state, senders, receivers, counts, border_rows, new_neighbours)
    return (vertex_state, edge_state)
```

```python
import jax
import jax.numpy as jnp
from jax import lax
from jax.sharding import PartitionSpec as P
from jax.experimental import pallas as pl
from jax.experimental.pallas import tpu as pltpu

F = 128
V = 256
E = 1536
CH = 256
EPS = 1e-05
f32 = jnp.float32
bf16 = jnp.bfloat16


def mm(a, b):
    return jnp.dot(a, b, preferred_element_type=f32)


def mm_nt(a, b):
    return lax.dot_general(a, b, (((1,), (1,)), ((), ())), preferred_element_type=f32)


def column(row):
    return jnp.broadcast_to(row, (F, F)).T


def flip(w):
    return w.astype(f32).T.astype(bf16)


def sublane_ids(rows):
    return lax.broadcasted_iota(jnp.int32, (rows, CH), 0).astype(f32).astype(bf16)


def one_hot(row, ids):
    return jnp.where(row == ids, jnp.ones((), bf16), jnp.zeros((), bf16))


def border_terms(terms, rows, ids):
    row = jnp.concatenate([rows[0:1], rows[1:2]], axis=1).astype(f32).astype(bf16)
    return mm(terms, one_hot(row, ids)).astype(bf16)


def start_kernel(perm, v_ref, border_ref, wn_ref, gy_ref, gx_ref):
    n = gy_ref.shape[0]
    wsT = flip(wn_ref[0, 0])
    ids = sublane_ids(V)
    for k in range(n):
        terms = mm_nt(wsT, v_ref[perm[k]]).astype(bf16)
        got = border_terms(terms, border_ref[perm[k]], ids)
        gy_ref[k] = got[:, :128]
        gx_ref[k] = got[:, 128:]


def step_kernel(perm, counts, v_ref, e_ref, gy_ref, gx_ref, s_ref, r_ref, border_ref,
                wi_ref, wn_ref, wo_ref, b_ref, g_ref, *rest, n, first, last):
    if last:
        out_ref, scr = rest[0], rest[1:]
    else:
        vo_ref, eo_ref, gyo_ref, gxo_ref = rest[:4]
        scr = rest[4:]
    wrT_s, wsT_s, woT_s, weT_s, cols_s, agg_s = scr
    k = pl.program_id(0)

    @pl.when(k == 0)
    def _():
        weT_s[...] = flip(wi_ref[0, 0])
        wsT_s[...] = flip(wi_ref[0, 1])
        wrT_s[...] = flip(wi_ref[0, 2])
        wo = wo_ref[0, 0].astype(f32)
        woT_s[...] = wo.T.astype(bf16)
        b1 = b_ref[0, 1:2]
        cols_s[0] = column(b_ref[0, 0:1])
        cols_s[1] = column(b1)
        cols_s[2] = column(g_ref[0, 0:1])
        cols_s[3] = column(b_ref[0, 2:3])

    src = perm[k]
    vrow = src if first else k
    v = v_ref[vrow]
    count = counts[src]
    own = mm_nt(wsT_s[...], v).astype(bf16)
    recv = mm_nt(wrT_s[...], v)
    b0 = cols_s[0]
    recv = recv.astype(bf16)
    ghost = jnp.concatenate([gy_ref[k], gx_ref[k]], axis=1)
    lhs_s = jnp.concatenate([own, ghost], axis=0)
    weT = weT_s[...]
    lhs_r = jnp.concatenate([
        jnp.concatenate([weT, recv[:, :128]], axis=1),
        jnp.concatenate([weT, recv[:, 128:]], axis=1)], axis=0)
    woT = woT_s[...]
    ids = sublane_ids(V)
    agg = None
    for c in range(E // CH):
        lo = c * CH
        s = s_ref[pl.ds(src, 1), lo:lo + CH]
        r = r_ref[pl.ds(src, 1), lo:lo + CH]
        live = (lax.broadcasted_iota(jnp.int32, (1, CH), 1) + lo) < count
        s_hi = s >= V
        r_hi = r >= 128
        s_low = jnp.where(s_hi, s - V, s).astype(f32).astype(bf16)
        r_low = jnp.where(r_hi, r - 128, r).astype(f32).astype(bf16)
        oh_s = one_hot(s_low, ids)
        oh_r = one_hot(r_low, ids[:128])
        if first:
            e_b = e_ref[0, lo:lo + CH, :].T
        else:
            e_b = e_ref[0, :, lo:lo + CH]
        e_f = e_b.astype(f32)
        sg = mm(lhs_s, oh_s)
        er = mm(lhs_r, jnp.concatenate([e_b, oh_r], axis=0))
        pre = jnp.where(s_hi, sg[128:], sg[:128]) + jnp.where(r_hi, er[128:], er[:128])
        pre = pre + jnp.concatenate([b0, b0], axis=1)
        h = jnp.maximum(pre, 0.0).astype(bf16)
        b1 = cols_s[1]
        center = mm(woT, h) + jnp.concatenate([b1, b1], axis=1)
        center = center - jnp.sum(center, axis=0, keepdims=True) * (1.0 / F)
        spread = jnp.sum(center * center, axis=0, keepdims=True) * (1.0 / F)
        inv = lax.rsqrt(spread + EPS)
        g, sh = cols_s[2], cols_s[3]
        upd = center * inv * jnp.concatenate([g, g], axis=1) + jnp.concatenate([sh, sh], axis=1)
        fresh = jnp.where(live, e_f + upd, e_f).astype(bf16)
        one = jnp.ones((), f32)
        zero = jnp.zeros((), f32)
        m_lo = jnp.where(jnp.logical_and(live, r < 128), one, zero).astype(bf16)
        m_hi = jnp.where(jnp.logical_and(live, r_hi), one, zero).astype(bf16)
        oh_v = jnp.concatenate([oh_r * m_lo, oh_r * m_hi], axis=0)
        part = mm_nt(oh_v, fresh)
        agg = part if agg is None else agg + part
        if last:
            rows = fresh.T
            for q in range(CH // 16):
                at = lo + q * 16
                out_ref[at // 48, k, at % 48:at % 48 + 16, :] = rows[q * 16:q * 16 + 16]
        else:
            eo_ref[0, :, lo:lo + CH] = fresh
    agg_s[k] = agg.astype(bf16)

    @pl.when(k == n - 1)
    def _():
        if first:
            vs = [v_ref[perm[i]] for i in range(n)]
        else:
            vs = [v_ref[i] for i in range(n)]
        vb = jnp.concatenate(vs, axis=0)
        ab = jnp.concatenate([agg_s[i] for i in range(n)], axis=0)
        wva = jnp.concatenate([wi_ref[0, 3], wi_ref[0, 4]], axis=0)
        hid = mm(jnp.concatenate([vb, ab], axis=1), wva) + b_ref[0, 3:4]
        hid = jnp.maximum(hid, 0.0).astype(bf16)
        center = mm(hid, wo_ref[0, 1]) + b_ref[0, 4:5]
        center = center - jnp.mean(center, axis=1, keepdims=True)
        spread = jnp.mean(center * center, axis=1, keepdims=True)
        upd = center * lax.rsqrt(spread + EPS) * g_ref[0, 1:2] + b_ref[0, 5:6]
        fresh_v = (vb.astype(f32) + upd).astype(bf16)
        if last:
            for i in range(n):
                for q in range(32):
                    at = i * V + q * 8
                    out_ref[q, i, 48:56, :] = fresh_v[at:at + 8]
        else:
            wnT = flip(wn_ref[0, 0])
            terms = mm_nt(wnT, fresh_v).astype(bf16)
            ids2 = sublane_ids(V)
            for i in range(n):
                vo_ref[i] = fresh_v[i * V:(i + 1) * V]
                got = border_terms(terms[:, i * V:(i + 1) * V], border_ref[perm[i]], ids2)
                gyo_ref[i] = got[:, :128]
                gxo_ref[i] = got[:, 128:]


def whole(shape):
    zeros = (0,) * len(shape)
    return pl.BlockSpec(tuple(shape), lambda *_: zeros)


def start_call(n, perm, v, border, w_in, interpret=False):
    return pl.pallas_call(
        start_kernel,
        grid_spec=pltpu.PrefetchScalarGridSpec(
            num_scalar_prefetch=1, grid=(1,),
            in_specs=[whole(v.shape), whole(border.shape),
                      pl.BlockSpec((1, 1, F, F), lambda *_: (0, 1, 0, 0))],
            out_specs=[whole((n, F, 128)), whole((n, F, 128))]),
        out_shape=[jax.ShapeDtypeStruct((n, F, 128), bf16)] * 2,
        interpret=interpret, name="start",
    )(perm, v, border, w_in)


def step_call(step, n, perm, counts, v, e, gy, gx, s, r, border, w_in, w_out, biases, gains,
              *, first, last, interpret=False):
    import functools
    nxt = min(step + 1, 2)
    if first:
        e_spec = pl.BlockSpec((1, E, F), lambda k, p, c: (p[k], 0, 0))
    else:
        e_spec = pl.BlockSpec((1, F, E), lambda k, p, c: (k, 0, 0))
    if last:
        out_specs = [whole((32, n, 56, F))]
        out_shape = [jax.ShapeDtypeStruct((32, n, 56, F), bf16)]
    else:
        out_specs = [whole((n, V, F)), pl.BlockSpec((1, F, E), lambda k, p, c: (k, 0, 0)),
                     whole((n, F, 128)), whole((n, F, 128))]
        out_shape = [jax.ShapeDtypeStruct((n, V, F), bf16), jax.ShapeDtypeStruct((n, F, E), bf16),
                     jax.ShapeDtypeStruct((n, F, 128), bf16), jax.ShapeDtypeStruct((n, F, 128), bf16)]
    return pl.pallas_call(
        functools.partial(step_kernel, n=n, first=first, last=last),
        grid_spec=pltpu.PrefetchScalarGridSpec(
            num_scalar_prefetch=2, grid=(n,),
            in_specs=[whole(v.shape), e_spec, whole(gy.shape), whole(gx.shape),
                      whole(s.shape), whole(r.shape), whole(border.shape),
                      pl.BlockSpec((1, 5, F, F), lambda *_: (step, 0, 0, 0)),
                      pl.BlockSpec((1, 1, F, F), lambda *_: (nxt, 1, 0, 0)),
                      pl.BlockSpec((1, 2, F, F), lambda *_: (step, 0, 0, 0)),
                      pl.BlockSpec((1, 6, F), lambda *_: (step, 0, 0)),
                      pl.BlockSpec((1, 2, F), lambda *_: (step, 0, 0))],
            out_specs=out_specs,
            scratch_shapes=[pltpu.VMEM((F, F), bf16)] * 4 + [
                pltpu.VMEM((4, F, F), f32), pltpu.VMEM((n, V, F), bf16)]),
        out_shape=out_shape,
        interpret=interpret, name=f"step{step}",
    )(perm, counts, v, e, gy, gx, s, r, border, w_in, w_in, w_out, biases, gains)


def roll_kernel(shifts, in_ref, out_ref):
    d = shifts[pl.program_id(0)]

    def body(j, carry):
        at = j + d
        at = jnp.where(at >= 32, at - 32, at)
        out_ref[at, 0] = in_ref[j, 0]
        return carry

    lax.fori_loop(0, 32, body, 0, unroll=4)


def roll_call(shifts, got):
    block = pl.BlockSpec((32, 1, 56, F), lambda k, d: (0, k, 0, 0))
    return pl.pallas_call(
        roll_kernel,
        grid_spec=pltpu.PrefetchScalarGridSpec(
            num_scalar_prefetch=1, grid=(got.shape[1],), in_specs=[block], out_specs=block),
        out_shape=jax.ShapeDtypeStruct(got.shape, bf16), name="roll",
    )(shifts, got)


def place_kernel(slots, in_ref, v_ref, e_ref):
    for q in range(32):
        e_ref[0, q * 48:q * 48 + 48, :] = in_ref[q, 0, :48, :]
        v_ref[0, q * 8:q * 8 + 8, :] = in_ref[q, 0, 48:, :]


def place_call(slots, got):
    n = got.shape[1]
    return pl.pallas_call(
        place_kernel,
        grid_spec=pltpu.PrefetchScalarGridSpec(
            num_scalar_prefetch=1, grid=(n,),
            in_specs=[pl.BlockSpec((32, 1, 56, F), lambda k, d: (0, k, 0, 0))],
            out_specs=[pl.BlockSpec((1, V, F), lambda k, d: (d[k], 0, 0)),
                       pl.BlockSpec((1, E, F), lambda k, d: (d[k], 0, 0))]),
        out_shape=[jax.ShapeDtypeStruct((n, V, F), bf16), jax.ShapeDtypeStruct((n, E, F), bf16)],
        name="place",
    )(slots, got)


def shifted(shard, axis):
    devices = lax.axis_size(axis)
    return lax.ppermute(shard, axis, [(i, (i + 1) % devices) for i in range(devices)])


def exchange(gy, gx):
    return shifted(gy, "gy"), shifted(gx, "gx")


def spread(values):
    return lax.all_to_all(values, "gy", split_axis=0, concat_axis=0, tiled=True)


def local(vertex_state, edge_state, senders, receivers, counts, border_rows, old_neighbours,
          new_neighbours, new_place, weights_in, weights_out, biases, norm_gains):
    n = vertex_state.shape[0]
    cycle = lax.axis_size("gy")
    me = lax.axis_index("gy")
    moved = ((new_place // n) % cycle - me) % cycle
    slots = jnp.arange(n, dtype=jnp.int32)
    order = moved * n + slots
    rank = jnp.sum((order[None, :] < order[:, None]).astype(jnp.int32), axis=1)
    chosen = (rank[None, :] == slots[:, None]).astype(jnp.int32)
    perm = jnp.sum(chosen * slots[None, :], axis=1)
    shifts = jnp.sum(chosen * moved[None, :], axis=1)
    landing = jnp.sum(chosen * (new_place % n)[None, :], axis=1)
    devices = jnp.arange(cycle, dtype=jnp.int32)
    goes = ((me + shifts) % cycle)[None, :] == devices[:, None]
    header = spread(jnp.sum(jnp.where(goes, landing[None, :], 0), axis=1))
    comes = ((me - shifts) % cycle)[:, None] == devices[None, :]
    landing = jnp.clip(jnp.sum(jnp.where(comes, header[None, :], 0), axis=1), 0, n - 1)

    rest = (senders, receivers, border_rows, weights_in, weights_out, biases, norm_gains)
    gy, gx = exchange(*start_call(n, perm, vertex_state, border_rows, weights_in))
    v, e, gy, gx = step_call(0, n, perm, counts, vertex_state, edge_state, gy, gx, *rest,
                             first=True, last=False)
    gy, gx = exchange(gy, gx)
    v, e, gy, gx = step_call(1, n, perm, counts, v, e, gy, gx, *rest, first=False, last=False)
    gy, gx = exchange(gy, gx)
    packed, = step_call(2, n, perm, counts, v, e, gy, gx, *rest, first=False, last=True)
    packed = spread(roll_call(shifts, spread(packed)))
    return tuple(place_call(landing, packed))


def solution(mesh):
    along = ("gx", "gy")
    placed = (P(along, None, None), P(along, None, None), P(along, None), P(along, None), P(along),
              P(along, None, None), P(along, None), P(along, None), P(along), P(), P(), P(), P())
    return jax.shard_map(
        local, mesh=mesh, in_specs=placed,
        out_specs=(P(along, None, None), P(along, None, None)), check_vma=False)
```
